32 devices in a mesh: shard: 8 (over y, x, core), tensor: 4 (over z).
Axes of the slice: x: 2, y: 2, z: 4, core: 2. Of those that a mesh axis runs over, the one named last changes fastest.
Arguments:
- tokens: bfloat16 [16384, 2048], P('shard'), may hold values from -40 to 40
- ln1_gain: bfloat16 [2048], P('shard'), may hold values from 0.25 to 1.75
- ln1_bias: bfloat16 [2048], P('shard'), may hold values from -3 to 3
- qkv_weight: bfloat16 [2048, 8, 3, 256], P('shard', 'tensor'), may hold values from -2 to 2
- qkv_bias: bfloat16 [8, 3, 256], P('tensor'), may hold values from -3 to 3
- out_weight: bfloat16 [2048, 8, 256], P('shard', 'tensor'), may hold values from -0.5 to 0.5
- out_bias: bfloat16 [2048], P('shard'), may hold values from -3 to 3
- ln2_gain: bfloat16 [2048], P('shard'), may hold values from 0.25 to 1.75
- ln2_bias: bfloat16 [2048], P('shard'), may hold values from -3 to 3
- fc1_weight: bfloat16 [2048, 8192], P('shard', 'tensor'), may hold values from -0.125 to 0.125
- fc1_bias: bfloat16 [8192], P('tensor'), may hold values from -3 to 3
- fc2_weight: bfloat16 [2048, 8192], P('shard', 'tensor'), may hold values from -0.0625 to 0.0625
- fc2_bias: bfloat16 [2048], P('shard'), may hold values from -3 to 3
- cotangent: bfloat16 [16384, 2048], P('shard'), may hold values from -6 to 6
Outputs:
- block_out: bfloat16 [16384, 2048], P('shard')
- grad_tokens: float32 [16384, 2048], P('shard')
- grad_ln1_gain: float32 [2048], P('shard')
- grad_ln1_bias: float32 [2048], P('shard')
- grad_qkv_weight: float32 [2048, 8, 3, 256], P('shard', 'tensor')
- grad_qkv_bias: float32 [8, 3, 256], P('tensor')
- grad_out_weight: float32 [2048, 8, 256], P('shard', 'tensor')
- grad_out_bias: float32 [2048], P('shard')
- grad_ln2_gain: float32 [2048], P('shard')
- grad_ln2_bias: float32 [2048], P('shard')
- grad_fc1_weight: float32 [2048, 8192], P('shard', 'tensor')
- grad_fc1_bias: float32 [8192], P('tensor')
- grad_fc2_weight: float32 [2048, 8192], P('shard', 'tensor')
- grad_fc2_bias: float32 [2048], P('shard')
The draws below stay inside these ranges and needn't reach their ends.
All inputs are finite; a program needn't handle non-finite values.
Results may differ from the reference program's by a relative error of at most 0.017.
Values may be sent and summed in bfloat16 or wider, within the bound.
A program may use at most 320 MiB of HBM per device.

```python
import math
import jax
import jax.numpy as jnp
from jax import lax

D = 2048
H = 8
HD = 256
ROT = 64
FF = 8192
SEQ = 256
SEQS = 64
TOKENS = 16384
N_TENSOR = 4


def draw_tokens(key, part):
    key_rows, key_cols, key_base = jax.random.split(key, 3)
    row_scale = jnp.exp(jax.random.uniform(key_rows, (TOKENS, 1), jnp.float32, math.log(0.3), math.log(3.0)))
    col_scale = jnp.exp(jax.random.uniform(key_cols, (1, D), jnp.float32, math.log(0.4), math.log(4.0)))
    base = jnp.clip(jax.random.normal(key_base, (TOKENS, D), jnp.float32), -6.0, 6.0)
    return jnp.clip(base * row_scale * col_scale, -40.0, 40.0).astype(jnp.bfloat16)


def draw_qkv_weight(key, part):
    key_main = jax.random.fold_in(key, 0)
    weight_scale = 1.0 / math.sqrt(D)
    main = jnp.clip(jax.random.normal(key_main, (D, H, 3, HD), jnp.float32), -4.0, 4.0) * weight_scale
    return jnp.clip(main, -2.0, 2.0).astype(jnp.bfloat16)


def steps_of(rng, shape, cuts, least, high):
    loudness, own = 1.0, jax.random.fold_in(rng, 6)
    for axis_at, blocks in cuts:
        heights = jnp.exp(jax.random.uniform(jax.random.fold_in(own, axis_at), (blocks,), jnp.float32, least / len(cuts), high / len(cuts)))
        loudness = loudness * jnp.repeat(heights, shape[axis_at] // blocks).reshape([-1 if axis == axis_at else 1 for axis in range(len(shape))])
    return loudness


def gaussian(rng, dims, scale, bound, pieces=(), kind=jnp.bfloat16):
    array = scale * jax.random.normal(rng, dims, jnp.float32)
    if pieces:
        array = array * steps_of(rng, dims, pieces, -0.22, 0.18)
    return jnp.clip(array, -bound, bound).astype(kind)


def setup_inputs(seed: int = 0) -> dict:
    keys = jax.random.split(jax.random.key(seed), 15)
    tokens = draw_tokens(jax.random.fold_in(keys[14], 71), 0)
    ln1_gain = jnp.clip(1.0 + 0.15 * jax.random.normal(keys[1], (D,), jnp.float32), 0.25, 1.75).astype(jnp.bfloat16)
    ln1_bias = gaussian(keys[2], (D,), 0.5, 3.0, ((0, 8),))
    qkv_weight = draw_qkv_weight(jax.random.fold_in(keys[14], 71), 0)
    qkv_bias = gaussian(keys[4], (H, 3, HD), 0.5, 3.0, ((0, 4),))
    out_weight = gaussian(keys[5], (D, H, HD), (D // 16) ** -0.5, 0.5, ((0, 8), (1, 4)))
    out_bias = gaussian(keys[6], (D,), 0.5, 3.0, ((0, 8),))
    ln2_gain = jnp.clip(1.0 + 0.15 * jax.random.normal(keys[7], (D,), jnp.float32), 0.25, 1.75).astype(jnp.bfloat16)
    ln2_bias = gaussian(keys[8], (D,), 0.5, 3.0, ((0, 8),))
    fc1_weight = gaussian(keys[9], (D, FF), D ** -0.5, 0.125, ((0, 8), (1, 4)))
    fc1_bias = gaussian(keys[10], (FF,), 0.5, 3.0, ((0, 4),))
    fc2_weight = gaussian(keys[11], (D, FF), FF ** -0.5, 0.0625, ((0, 8), (1, 4)))
    fc2_bias = gaussian(keys[12], (D,), 0.5, 3.0, ((0, 8),))
    cotangent = gaussian(keys[13], (TOKENS, D), 1.0, 6.0, ((0, 8),))
    return dict(tokens=tokens, ln1_gain=ln1_gain, ln1_bias=ln1_bias, qkv_weight=qkv_weight, qkv_bias=qkv_bias, out_weight=out_weight, out_bias=out_bias, ln2_gain=ln2_gain, ln2_bias=ln2_bias, fc1_weight=fc1_weight, fc1_bias=fc1_bias, fc2_weight=fc2_weight, fc2_bias=fc2_bias, cotangent=cotangent)


NORM_EPS = 1e-05
ROOT_HALF = 0.7071067811865476
INV_ROOT_TWO_PI = 0.3989422804014327

def normalize(residual):
    row_mean = lax.optimization_barrier(jnp.mean(residual, axis=-1, keepdims=True))
    centered = residual - row_mean
    row_var = lax.optimization_barrier(jnp.mean(centered * centered, axis=-1, keepdims=True))
    inv_std = lax.rsqrt(row_var + NORM_EPS)
    return (centered * inv_std, inv_std)

def norm_backward(grad_normed, gain_wide, normalized, inv_std):
    scaled_grad = grad_normed * gain_wide
    return inv_std * (scaled_grad - lax.optimization_barrier(jnp.mean(scaled_grad, axis=-1, keepdims=True)) - normalized * lax.optimization_barrier(jnp.mean(scaled_grad * normalized, axis=-1, keepdims=True)))

def rotary_tables(length, rot_dims):
    half_dims = rot_dims // 2
    frequency = jnp.power(10000.0, -2.0 * jnp.arange(half_dims, dtype=jnp.float32) / rot_dims)
    angles = jnp.arange(length, dtype=jnp.float32)[:, None] * frequency[None, :]
    return (jnp.cos(angles), jnp.sin(angles))

def rotate(field, cos_tab, sin_tab, rot_dims):
    half_dims = rot_dims // 2
    lower_half = field[..., :half_dims]
    upper_half = field[..., half_dims:rot_dims]
    cos_wide = cos_tab[None, :, None, :]
    sin_wide = sin_tab[None, :, None, :]
    return jnp.concatenate([lower_half * cos_wide - upper_half * sin_wide, upper_half * cos_wide + lower_half * sin_wide, field[..., rot_dims:]], axis=-1)

def rotate_back(grad_field, cos_tab, sin_tab, rot_dims):
    half_dims = rot_dims // 2
    lower_half = grad_field[..., :half_dims]
    upper_half = grad_field[..., half_dims:rot_dims]
    cos_wide = cos_tab[None, :, None, :]
    sin_wide = sin_tab[None, :, None, :]
    return jnp.concatenate([lower_half * cos_wide + upper_half * sin_wide, upper_half * cos_wide - lower_half * sin_wide, grad_field[..., rot_dims:]], axis=-1)

def gelu_exact(pre_act):
    return 0.5 * pre_act * (1.0 + lax.erf(pre_act * ROOT_HALF))

def gelu_slope(pre_act):
    return 0.5 * (1.0 + lax.erf(pre_act * ROOT_HALF)) + pre_act * jnp.exp(-0.5 * pre_act * pre_act) * INV_ROOT_TWO_PI

def wide_einsum(form, left_op, right_op):
    return jnp.einsum(form, left_op.astype(jnp.float32), right_op.astype(jnp.float32), precision=lax.Precision.HIGHEST)

def causal_scores(queries, key_rows, score_scale):
    length = queries.shape[1]
    scores = wide_einsum('nqhc,nkhc->nhqk', queries, key_rows) * score_scale
    causal = jnp.arange(length)[:, None] >= jnp.arange(length)[None, :]
    return jnp.where(causal[None, None], scores, -1e+30)

def layer_block(params, x_block, grad_block):
    ln1_gain, ln1_bias, qkv_weight, qkv_bias, out_weight, out_bias, ln2_gain, ln2_bias, fc1_weight, fc1_bias, fc2_weight, fc2_bias = params
    row_count = x_block.shape[0]
    seq_count = row_count // SEQ
    residual = x_block.astype(jnp.float32)
    normalized, inv_std = normalize(residual)
    gain_one = ln1_gain.astype(jnp.float32)
    gain_two = ln2_gain.astype(jnp.float32)
    normed_one = (normalized * gain_one + ln1_bias.astype(jnp.float32)).astype(jnp.bfloat16)
    normed_two = (normalized * gain_two + ln2_bias.astype(jnp.float32)).astype(jnp.bfloat16)
    qkv_flat = qkv_weight.reshape(D, H * 3 * HD)
    qkv = jnp.dot(normed_one, qkv_flat, preferred_element_type=jnp.float32).reshape(row_count, H, 3, HD)
    qkv = qkv + qkv_bias.astype(jnp.float32)
    fields = qkv.reshape(seq_count, SEQ, H, 3, HD)
    cos_tab, sin_tab = rotary_tables(SEQ, ROT)
    queries = rotate(fields[:, :, :, 0], cos_tab, sin_tab, ROT).astype(jnp.bfloat16)
    key_rows = rotate(fields[:, :, :, 1], cos_tab, sin_tab, ROT).astype(jnp.bfloat16)
    values = fields[:, :, :, 2].astype(jnp.bfloat16)
    score_scale = 1.0 / math.sqrt(HD)
    scores = causal_scores(queries, key_rows, score_scale)
    row_top = lax.optimization_barrier(jnp.max(scores, axis=-1, keepdims=True))
    log_total = row_top + jnp.log(lax.optimization_barrier(jnp.sum(jnp.exp(scores - row_top), axis=-1, keepdims=True)))
    attn_probs = jnp.exp(scores - log_total).astype(jnp.bfloat16)
    attn_out = wide_einsum('nhqk,nkhc->nqhc', attn_probs, values).astype(jnp.bfloat16)
    attn_out = attn_out.reshape(row_count, H * HD)
    out_flat = out_weight.reshape(D, H * HD)
    pre_act = jnp.dot(normed_two, fc1_weight, preferred_element_type=jnp.float32) + fc1_bias.astype(jnp.float32)
    hidden = gelu_exact(pre_act).astype(jnp.bfloat16)
    head_width = H // N_TENSOR * HD
    unit_width = FF // N_TENSOR
    branch_total = jnp.zeros((row_count, D), jnp.float32)
    for tensor_idx in range(N_TENSOR):
        head_lo = tensor_idx * head_width
        unit_lo = tensor_idx * unit_width
        partial_value = jnp.dot(attn_out[:, head_lo:head_lo + head_width], out_flat[:, head_lo:head_lo + head_width].T, preferred_element_type=jnp.float32)
        partial_value = partial_value + jnp.dot(hidden[:, unit_lo:unit_lo + unit_width], fc2_weight[:, unit_lo:unit_lo + unit_width].T, preferred_element_type=jnp.float32)
        branch_total = branch_total + lax.optimization_barrier(partial_value.astype(jnp.bfloat16)).astype(jnp.float32)
    block_out = (residual + branch_total + out_bias.astype(jnp.float32) + fc2_bias.astype(jnp.float32)).astype(jnp.bfloat16)
    grad_wide = grad_block.astype(jnp.float32)
    shift_grad = lax.optimization_barrier(jnp.sum(grad_wide, axis=0))
    grad_out_w = jnp.dot(grad_block.T, attn_out, preferred_element_type=jnp.float32).reshape(D, H, HD)
    grad_fc2_w = jnp.dot(grad_block.T, hidden, preferred_element_type=jnp.float32)
    d_attn = jnp.dot(grad_block, out_flat, preferred_element_type=jnp.float32).astype(jnp.bfloat16)
    d_attn = d_attn.reshape(seq_count, SEQ, H, HD)
    d_pre = jnp.dot(grad_block, fc2_weight, preferred_element_type=jnp.float32) * gelu_slope(pre_act)
    grad_fc1_b = lax.optimization_barrier(jnp.sum(d_pre, axis=0))
    d_pre_b = d_pre.astype(jnp.bfloat16)
    grad_fc1_w = jnp.dot(normed_two.T, d_pre_b, preferred_element_type=jnp.float32)
    d_two = jnp.dot(d_pre_b, fc1_weight.T, preferred_element_type=jnp.float32)
    probs_again = jnp.exp(causal_scores(queries, key_rows, score_scale) - log_total)
    d_values = wide_einsum('nhqk,nqhc->nkhc', probs_again.astype(jnp.bfloat16), d_attn)
    d_probs = wide_einsum('nqhc,nkhc->nhqk', d_attn, values)
    row_delta = lax.optimization_barrier(jnp.sum(probs_again * d_probs, axis=-1, keepdims=True))
    d_scores = (probs_again * (d_probs - row_delta) * score_scale).astype(jnp.bfloat16)
    d_queries = rotate_back(wide_einsum('nhqk,nkhc->nqhc', d_scores, key_rows), cos_tab, sin_tab, ROT)
    d_keys = rotate_back(wide_einsum('nhqk,nqhc->nkhc', d_scores, queries), cos_tab, sin_tab, ROT)
    d_qkv = jnp.stack([d_queries, d_keys, d_values], axis=3).reshape(row_count, H, 3, HD)
    grad_qkv_b = lax.optimization_barrier(jnp.sum(d_qkv, axis=0))
    d_qkv_b = d_qkv.astype(jnp.bfloat16).reshape(row_count, H * 3 * HD)
    grad_qkv_w = jnp.dot(normed_one.T, d_qkv_b, preferred_element_type=jnp.float32).reshape(D, H, 3, HD)
    d_one = jnp.dot(d_qkv_b, qkv_flat.T, preferred_element_type=jnp.float32)
    grad_g1 = lax.optimization_barrier(jnp.sum(d_one * normalized, axis=0))
    grad_b1 = lax.optimization_barrier(jnp.sum(d_one, axis=0))
    grad_g2 = lax.optimization_barrier(jnp.sum(d_two * normalized, axis=0))
    grad_b2 = lax.optimization_barrier(jnp.sum(d_two, axis=0))
    grad_rows = grad_wide + norm_backward(d_one, gain_one, normalized, inv_std) + norm_backward(d_two, gain_two, normalized, inv_std)
    grads = (grad_g1, grad_b1, grad_qkv_w, grad_qkv_b, grad_out_w, shift_grad, grad_g2, grad_b2, grad_fc1_w, grad_fc1_b, grad_fc2_w, shift_grad)
    return (block_out, grad_rows, grads)

def reference(tokens, ln1_gain, ln1_bias, qkv_weight, qkv_bias, out_weight, out_bias, ln2_gain, ln2_bias, fc1_weight, fc1_bias, fc2_weight, fc2_bias, cotangent):
    params = (ln1_gain, ln1_bias, qkv_weight, qkv_bias, out_weight, out_bias, ln2_gain, ln2_bias, fc1_weight, fc1_bias, fc2_weight, fc2_bias)
    block_seqs = math.gcd(SEQS, max(1, 4096 // SEQ))
    block_rows = block_seqs * SEQ
    block_count = TOKENS // block_rows
    x_blocks = tokens.reshape(block_count, block_rows, D)
    g_blocks = cotangent.reshape(block_count, block_rows, D)
    zero_grads = (jnp.zeros((D,), jnp.float32), jnp.zeros((D,), jnp.float32), jnp.zeros((D, H, 3, HD), jnp.float32), jnp.zeros((H, 3, HD), jnp.float32), jnp.zeros((D, H, HD), jnp.float32), jnp.zeros((D,), jnp.float32), jnp.zeros((D,), jnp.float32), jnp.zeros((D,), jnp.float32), jnp.zeros((D, FF), jnp.float32), jnp.zeros((FF,), jnp.float32), jnp.zeros((D, FF), jnp.float32), jnp.zeros((D,), jnp.float32))

    def scan_step(grad_accum, block_pair):
        x_block, grad_block = block_pair
        block_out, grad_rows, grads = layer_block(params, x_block, grad_block)
        summed = tuple((older + newer for older, newer in zip(grad_accum, grads)))
        return (summed, (block_out, grad_rows))
    grad_accum, (out_blocks, grad_blocks) = lax.scan(scan_step, zero_grads, (x_blocks, g_blocks))
    grad_g1, grad_b1, grad_qkv_w, grad_qkv_b, grad_out_w, grad_out_b, grad_g2, grad_b2, grad_fc1_w, grad_fc1_b, grad_fc2_w, grad_fc2_b = grad_accum
    return (out_blocks.reshape(TOKENS, D), grad_blocks.reshape(TOKENS, D), grad_g1, grad_b1, grad_qkv_w, grad_qkv_b, grad_out_w, grad_out_b, grad_g2, grad_b2, grad_fc1_w, grad_fc1_b, grad_fc2_w, grad_fc2_b)
```

```python
import functools
import math

import jax
import jax.numpy as jnp
from jax import lax
from jax.experimental import pallas as pl
from jax.experimental.pallas import tpu as pltpu
from jax.sharding import PartitionSpec as P


ROT = 64
SEQ = 256
CORES = 2
LANES = 128
FWD_PARTS = (4, 4, 4, 4)
BWD_PARTS = (4, 4, 4, 4)
LAST_PARTS = (1,)
VMEM_LIMIT = 60 << 20


NORM_EPS = 1e-05
ROOT_HALF = 0.7071067811865476
INV_ROOT_TWO_PI = 0.3989422804014327
MESH = pl.DeviceIdType.MESH


def normalize(residual):
    row_mean = jnp.mean(residual, axis=-1, keepdims=True)
    centered = residual - row_mean
    row_var = jnp.mean(centered * centered, axis=-1, keepdims=True)
    inv_std = lax.rsqrt(row_var + NORM_EPS)
    return (centered * inv_std, inv_std)


def norm_backward(grad_normed, gain_wide, normalized, inv_std):
    scaled_grad = grad_normed * gain_wide
    return inv_std * (
        scaled_grad
        - jnp.mean(scaled_grad, axis=-1, keepdims=True)
        - normalized * jnp.mean(scaled_grad * normalized, axis=-1, keepdims=True)
    )


def gelu_exact(pre_act):
    return 0.5 * pre_act * (1.0 + lax.erf(pre_act * ROOT_HALF))


def gelu_slope(pre_act):
    return (
        0.5 * (1.0 + lax.erf(pre_act * ROOT_HALF))
        + pre_act * jnp.exp(-0.5 * pre_act * pre_act) * INV_ROOT_TWO_PI
    )


def rotary_tables(length, rot_dims):
    half_dims = rot_dims // 2
    frequency = jnp.power(10000.0, -2.0 * jnp.arange(half_dims, dtype=jnp.float32) / rot_dims)
    angles = jnp.arange(length, dtype=jnp.float32)[:, None] * frequency[None, :]
    cos_tab, sin_tab = jnp.cos(angles), jnp.sin(angles)
    zeros = jnp.zeros((length, half_dims), jnp.float32)
    rest = jnp.zeros((length, LANES - rot_dims), jnp.float32)
    keep = jnp.concatenate([cos_tab, cos_tab, rest + 1.0], axis=1)
    from_upper = jnp.concatenate([-sin_tab, zeros, rest], axis=1)
    from_lower = jnp.concatenate([zeros, sin_tab, rest], axis=1)
    return jnp.stack([keep, from_upper, from_lower])


def rotate(field, table_ref, sign):
    first = field[:, :LANES]
    half_dims = ROT // 2
    turned = (
        first * table_ref[0]
        + sign * pltpu.roll(first, LANES - half_dims, 1) * table_ref[1]
        + sign * pltpu.roll(first, half_dims, 1) * table_ref[2]
    )
    return jnp.concatenate([turned, field[:, LANES:]], axis=1)


def dot_nn(left, right):
    return jnp.dot(left, right, preferred_element_type=jnp.float32)


def dot_nt(left, right):
    return lax.dot_general(left, right, (((1,), (1,)), ((), ())), preferred_element_type=jnp.float32)


def dot_tn(left, right):
    return lax.dot_general(left, right, (((0,), (0,)), ((), ())), preferred_element_type=jnp.float32)


def probabilities(queries, key_rows, score_scale):
    scores = dot_nt(queries, key_rows) * score_scale
    length = scores.shape[0]
    row_at = lax.broadcasted_iota(jnp.int32, (length, length), 0)
    key_at = lax.broadcasted_iota(jnp.int32, (length, length), 1)
    scores = jnp.where(row_at >= key_at, scores, -1e30)
    row_top = jnp.max(scores, axis=-1, keepdims=True)
    weights = jnp.exp(scores - row_top)
    return weights * (1.0 / jnp.sum(weights, axis=-1, keepdims=True))


def call(kernel, grid, in_specs, out_specs, out_shape, flops, moved, **more):
    return pl.pallas_call(
        kernel,
        grid=grid,
        in_specs=in_specs,
        out_specs=out_specs,
        out_shape=out_shape,
        compiler_params=pltpu.CompilerParams(vmem_limit_bytes=VMEM_LIMIT),
        cost_estimate=pl.CostEstimate(flops=flops, bytes_accessed=moved, transcendentals=0),
        **more,
    )


def whole(shape):
    return pl.BlockSpec(
        shape, lambda step: (0,) * len(shape), pipeline_mode=pl.Buffered(1)
    )


def by_rows(rows, columns, first=0):
    return pl.BlockSpec((rows, columns), lambda step: (step + first, 0))


def attention_block(
    x_ref,
    vec_ref,
    weight_ref,
    shift_ref,
    table_ref,
    one_ref,
    two_ref,
    qkv_ref,
    attn_ref,
    head_count,
    head_dim,
):
    score_scale = 1.0 / math.sqrt(head_dim)
    normalized, _ = normalize(x_ref[...].astype(jnp.float32))
    one = (normalized * vec_ref[0:1] + vec_ref[1:2]).astype(jnp.bfloat16)
    one_ref[...] = one
    two_ref[...] = (normalized * vec_ref[2:3] + vec_ref[3:4]).astype(jnp.bfloat16)
    for head in range(head_count):
        fields = []
        for kind in range(3):
            at = slice((head * 3 + kind) * head_dim, (head * 3 + kind + 1) * head_dim)
            field = dot_nn(one, weight_ref[:, at]) + shift_ref[:, at]
            if kind < 2:
                field = rotate(field, table_ref, 1.0)
            field = field.astype(jnp.bfloat16)
            qkv_ref[:, at] = field
            fields.append(field)
        probs = probabilities(fields[0], fields[1], score_scale).astype(jnp.bfloat16)
        attn_ref[:, head * head_dim : (head + 1) * head_dim] = dot_nn(probs, fields[2]).astype(
            jnp.bfloat16
        )


def attention_forward(tokens, vectors, qkv_full, qkv_shift, table, head_count, head_dim):
    row_count, width = tokens.shape
    qkv_width = qkv_full.shape[1]

    def kernel(x_ref, vec_ref, weight_ref, shift_ref, table_ref, *out_refs):
        attention_block(
            x_ref, vec_ref, weight_ref, shift_ref, table_ref, *out_refs, head_count, head_dim
        )

    attn_width = head_count * head_dim
    return call(
        kernel,
        (row_count // SEQ,),
        [
            by_rows(SEQ, width),
            whole(vectors.shape),
            whole(qkv_full.shape),
            whole(qkv_shift.shape),
            whole(table.shape),
        ],
        [
            by_rows(SEQ, width),
            by_rows(SEQ, width),
            by_rows(SEQ, qkv_width),
            by_rows(SEQ, attn_width),
        ],
        [
            jax.ShapeDtypeStruct((row_count, width), jnp.bfloat16),
            jax.ShapeDtypeStruct((row_count, width), jnp.bfloat16),
            jax.ShapeDtypeStruct((row_count, qkv_width), jnp.bfloat16),
            jax.ShapeDtypeStruct((row_count, attn_width), jnp.bfloat16),
        ],
        2 * row_count * width * qkv_width,
        2 * (3 * row_count * width + width * qkv_width + row_count * (qkv_width + attn_width)),
        name="attention_forward",
    )(tokens, vectors, qkv_full, qkv_shift, table)


def attention_backward(cotangent, out_full, qkv, table, head_count, head_dim):
    row_count, width = cotangent.shape
    qkv_width = qkv.shape[1]
    attn_width = head_count * head_dim
    score_scale = 1.0 / math.sqrt(head_dim)

    def kernel(grad_ref, out_ref, qkv_ref, table_ref, d_qkv_ref, shift_ref, sum_ref):
        @pl.when(pl.program_id(0) == 0)
        def _():
            shift_ref[...] = jnp.zeros_like(shift_ref)
            sum_ref[...] = jnp.zeros_like(sum_ref)

        grad = grad_ref[...]
        sum_ref[0:1] += jnp.sum(grad.astype(jnp.float32), axis=0, keepdims=True)
        for head in range(head_count):
            d_attn = dot_nn(grad, out_ref[:, head * head_dim : (head + 1) * head_dim])
            d_attn = d_attn.astype(jnp.bfloat16)
            at = [
                slice((head * 3 + kind) * head_dim, (head * 3 + kind + 1) * head_dim)
                for kind in range(3)
            ]
            queries, key_rows, values = (qkv_ref[:, part] for part in at)
            probs = probabilities(queries, key_rows, score_scale)
            d_values = dot_tn(probs.astype(jnp.bfloat16), d_attn)
            d_probs = dot_nt(d_attn, values)
            row_delta = jnp.sum(probs * d_probs, axis=-1, keepdims=True)
            d_scores = (probs * (d_probs - row_delta) * score_scale).astype(jnp.bfloat16)
            d_queries = rotate(dot_nn(d_scores, key_rows), table_ref, -1.0)
            d_keys = rotate(dot_tn(d_scores, queries), table_ref, -1.0)
            for part, value in zip(at, (d_queries, d_keys, d_values)):
                d_qkv_ref[:, part] = value.astype(jnp.bfloat16)
                shift_ref[0:1, part] += jnp.sum(value, axis=0, keepdims=True)

    return call(
        kernel,
        (row_count // SEQ,),
        [by_rows(SEQ, width), whole(out_full.shape), by_rows(SEQ, qkv_width), whole(table.shape)],
        [
            by_rows(SEQ, qkv_width),
            pl.BlockSpec((8, qkv_width), lambda step: (0, 0)),
            pl.BlockSpec((8, width), lambda step: (0, 0)),
        ],
        [
            jax.ShapeDtypeStruct((row_count, qkv_width), jnp.bfloat16),
            jax.ShapeDtypeStruct((8, qkv_width), jnp.float32),
            jax.ShapeDtypeStruct((8, width), jnp.float32),
        ],
        2 * row_count * width * attn_width + 10 * row_count * SEQ * attn_width,
        2 * (row_count * width + width * attn_width + 2 * row_count * qkv_width),
        name="attention_backward",
    )(cotangent, out_full, qkv, table)


def branch_part(attn_out, hidden, out_full, fc2_full, first, rows):
    width = out_full.shape[0]

    def kernel(attn_ref, hidden_ref, out_ref, fc2_ref, part_ref):
        total = dot_nt(attn_ref[...], out_ref[...]) + dot_nt(hidden_ref[...], fc2_ref[...])
        part_ref[...] = total.astype(jnp.bfloat16)

    inner = attn_out.shape[1] + hidden.shape[1]
    return call(
        kernel,
        (rows // SEQ,),
        [
            by_rows(SEQ, attn_out.shape[1], first // SEQ),
            by_rows(SEQ, hidden.shape[1], first // SEQ),
            whole(out_full.shape),
            whole(fc2_full.shape),
        ],
        by_rows(SEQ, width),
        jax.ShapeDtypeStruct((rows, width), jnp.bfloat16),
        2 * rows * width * inner,
        2 * (rows * (width + inner) + width * inner),
        name="branch_part",
    )(attn_out, hidden, out_full, fc2_full)


def input_grad(d_pre, d_qkv, tokens, vectors, fc1_full, qkv_full, first, rows):
    width = tokens.shape[1]

    def kernel(pre_ref, qkv_ref, x_ref, vec_ref, fc1_ref, weight_ref, grad_ref, terms_ref):
        @pl.when(pl.program_id(0) == 0)
        def _():
            terms_ref[...] = jnp.zeros_like(terms_ref)

        normalized, inv_std = normalize(x_ref[...].astype(jnp.float32))
        d_one = dot_nt(qkv_ref[...], weight_ref[...])
        terms_ref[0:1] += jnp.sum(d_one * normalized, axis=0, keepdims=True)
        terms_ref[1:2] += jnp.sum(d_one, axis=0, keepdims=True)
        d_two = dot_nt(pre_ref[...], fc1_ref[...])
        terms_ref[2:3] += jnp.sum(d_two * normalized, axis=0, keepdims=True)
        terms_ref[3:4] += jnp.sum(d_two, axis=0, keepdims=True)
        joined = d_one * vec_ref[0:1] + d_two * vec_ref[2:3]
        grad_ref[...] = norm_backward(joined, 1.0, normalized, inv_std).astype(jnp.bfloat16)

    inner = d_pre.shape[1] + d_qkv.shape[1]
    return call(
        kernel,
        (rows // SEQ,),
        [
            by_rows(SEQ, d_pre.shape[1], first // SEQ),
            by_rows(SEQ, d_qkv.shape[1], first // SEQ),
            by_rows(SEQ, width, first // SEQ),
            whole(vectors.shape),
            whole(fc1_full.shape),
            whole(qkv_full.shape),
        ],
        [by_rows(SEQ, width), pl.BlockSpec((8, width), lambda step: (0, 0))],
        [
            jax.ShapeDtypeStruct((rows, width), jnp.bfloat16),
            jax.ShapeDtypeStruct((8, width), jnp.float32),
        ],
        2 * rows * width * inner,
        2 * (rows * (2 * width + inner) + width * inner),
        name="input_grad",
    )(d_pre, d_qkv, tokens, vectors, fc1_full, qkv_full)


def chip_at(place, chips):
    if chips & (chips - 1):
        return place
    chip, bit = 0, 1
    while bit < chips:
        chip = chip + bit * lax.rem(place // bit + place // (2 * bit), 2)
        bit *= 2
    return chip


def place_of(chip, chips):
    if chips & (chips - 1):
        return chip
    place, bit = 0, 1
    while bit < chips:
        ones, higher = 0, bit
        while higher < chips:
            ones = ones + chip // higher
            higher *= 2
        place = place + bit * lax.rem(ones, 2)
        bit *= 2
    return place


def ring_serves(shards):
    chips = shards // CORES
    return shards % CORES == 0 and chips % 2 == 0 and chips >= 4


def gather_forward(parts, tokens, qkv_shift, fc1_shift, table, shards, head_count, head_dim):
    chips = shards // CORES
    count = len(parts)
    hops = chips // 2 - 1
    kinds = 2 * hops + 2
    total_kinds = kinds + 1 + kinds
    row_count, width = tokens.shape
    own_rows, qkv_width = parts[1].shape
    units = parts[2].shape[1]
    attn_width = head_count * head_dim

    def kernel(*refs):
        own = refs[:count]
        x_ref, qkv_shift_ref, fc1_shift_ref, table_ref = refs[count : count + 4]
        full = refs[count + 4 : 2 * count + 4]
        one_ref, two_ref, qkv_ref, attn_ref, hidden_ref, pre_ref = refs[2 * count + 4 : 2 * count + 10]
        vec_buf, vec_rows, qkv_buf, fc1_buf, send_sems, recv_sems, keep_sems, load_sems = refs[
            2 * count + 10 :
        ]
        me = lax.axis_index("shard")
        core = lax.rem(me, CORES)
        place = place_of(me // CORES, chips)

        def shard_at(shift, flip=0):
            there = chip_at(lax.rem(place + shift + chips, chips), chips)
            return there * CORES + (1 - core if flip else core)

        right, left, peer = shard_at(1), shard_at(-1), shard_at(0, 1)
        barrier = pltpu.get_barrier_semaphore()
        for target in (right, left, peer):
            pl.semaphore_signal(barrier, inc=1, device_id={"shard": target}, device_id_type=MESH)
        pl.semaphore_wait(barrier, 3)
        copies = {}

        def send(index, kind, src, dst, target):
            copy = pltpu.make_async_remote_copy(
                src_ref=src,
                dst_ref=dst,
                send_sem=send_sems.at[index, kind],
                recv_sem=recv_sems.at[index, kind],
                device_id={"shard": target},
                device_id_type=MESH,
            )
            copy.start()
            copies[index, kind] = copy

        def half(which, index):
            rows = own[index].shape[0] // 2
            return pl.ds(which * rows, rows)

        def across(index, kind, piece):
            send(index, kinds + 1 + kind, piece, piece, peer)

        def keep(index):
            return pltpu.make_async_copy(own[index], full[index].at[me], keep_sems.at[index])

        def begin(*indices):
            for index in indices:
                mine = full[index].at[me]
                send(index, 0, own[index], mine, right)
                send(index, hops, own[index], mine, left)
                send(index, kinds, own[index], mine, peer)
                keep(index).start()

        def forward(*indices):
            for hop in range(hops):
                for index in indices:
                    for kind, sign, target in ((hop, -1, right), (hops + hop, 1, left)):
                        copies[index, kind].wait_recv()
                        shard = shard_at(sign * (hop + 1))
                        piece = full[index].at[shard]
                        if hop + 1 < hops:
                            send(index, kind + 1, piece, piece, target)
                        else:
                            which = 0 if sign < 0 else 1
                            part = full[index].at[shard, half(which, index)]
                            send(index, 2 * hops + which, part, part, target)
                        across(index, kind, piece)

        def finish(*indices):
            for index in indices:
                for which in range(2):
                    last = 2 * hops + which
                    copies[index, last].wait_recv()
                    across(index, last, full[index].at[shard_at(chips // 2), half(which, index)])
            for index in indices:
                for kind in range(kinds, total_kinds):
                    copies[index, kind].wait_recv()
                for kind in range(total_kinds):
                    copies[index, kind].wait_send()
                keep(index).wait()

        def load(index, buffer, slot):
            loads = [
                pltpu.make_async_copy(
                    full[index].at[shard],
                    buffer.at[pl.ds(shard * own[index].shape[0], own[index].shape[0])],
                    load_sems.at[slot + shard],
                )
                for shard in range(shards)
            ]
            for one in loads:
                one.start()
            for one in loads:
                one.wait()

        def rows_of(columns):
            return pl.BlockSpec((SEQ, columns), lambda step: (step, 0))

        begin(0, 1)
        forward(0, 1)
        begin(2, 3)
        finish(0, 1)
        load(0, vec_buf, 0)
        load(1, qkv_buf, shards)
        for shard in range(shards):
            vec_rows[:, shard * own_rows : (shard + 1) * own_rows] = vec_buf[
                shard * 16 : (shard + 1) * 16
            ].astype(jnp.float32)

        def attend(*blocks):
            attention_block(
                blocks[0],
                vec_rows,
                qkv_buf,
                qkv_shift_ref,
                table_ref,
                *blocks[1:],
                head_count,
                head_dim,
            )

        pltpu.emit_pipeline(
            attend,
            grid=(row_count // SEQ,),
            in_specs=[rows_of(width)],
            out_specs=[rows_of(width), rows_of(width), rows_of(qkv_width), rows_of(attn_width)],
        )(x_ref, one_ref, two_ref, qkv_ref, attn_ref)

        forward(2, 3)
        begin(4)
        finish(2)
        load(2, fc1_buf, 2 * shards)

        def feed(two_block, hidden_block, pre_block):
            tile = min(units, 512)
            for at in range(0, units, tile):
                cut = slice(at, at + tile)
                pre = dot_nn(two_block[...], fc1_buf[:, cut]) + fc1_shift_ref[:, cut]
                pre_block[:, cut] = pre
                hidden_block[:, cut] = gelu_exact(pre).astype(jnp.bfloat16)

        pltpu.emit_pipeline(
            feed,
            grid=(row_count // SEQ,),
            in_specs=[rows_of(width)],
            out_specs=[rows_of(units), rows_of(units)],
        )(two_ref, hidden_ref, pre_ref)

        forward(4)
        finish(3, 4)

    sent = sum(part.size * part.dtype.itemsize for part in parts)
    any_space = pl.BlockSpec(memory_space=pl.ANY)
    in_vmem = pl.BlockSpec(memory_space=pltpu.VMEM)
    shapes = [((shards,) + part.shape, part.dtype) for part in parts] + [
        ((row_count, width), jnp.bfloat16),
        ((row_count, width), jnp.bfloat16),
        ((row_count, qkv_width), jnp.bfloat16),
        ((row_count, attn_width), jnp.bfloat16),
        ((row_count, units), jnp.bfloat16),
        ((row_count, units), jnp.float32),
    ]
    results = pl.pallas_call(
        kernel,
        in_specs=[in_vmem] * count + [any_space] + [in_vmem] * 3,
        out_specs=[any_space] * len(shapes),
        out_shape=[jax.ShapeDtypeStruct(*shape) for shape in shapes],
        scratch_shapes=[
            pltpu.VMEM((shards * 16, own_rows), jnp.bfloat16),
            pltpu.VMEM((16, width), jnp.float32),
            pltpu.VMEM((width, qkv_width), jnp.bfloat16),
            pltpu.VMEM((width, units), jnp.bfloat16),
            pltpu.SemaphoreType.DMA((count, total_kinds)),
            pltpu.SemaphoreType.DMA((count, total_kinds)),
            pltpu.SemaphoreType.DMA((count,)),
            pltpu.SemaphoreType.DMA((3 * shards,)),
        ],
        compiler_params=pltpu.CompilerParams(
            collective_id=0, has_side_effects=True, vmem_limit_bytes=VMEM_LIMIT
        ),
        cost_estimate=pl.CostEstimate(
            flops=2 * row_count * width * (qkv_width + units),
            bytes_accessed=2 * shards * sent + 18 * row_count * width,
            transcendentals=row_count * units,
        ),
        name="gather_forward",
    )(*parts, tokens, qkv_shift, fc1_shift, table)
    return results[:count], results[count:]


def line_sum(part, count):
    if count == 1:
        return part
    if count % 2:
        return lax.psum(part, "tensor")
    me = lax.axis_index("tensor")
    middle = count // 2
    total = part
    for step in range(count - 1):
        if step < middle:
            moves = [(step, step + 1), (count - 1 - step, count - 2 - step)]
        else:
            near = count - 2 - step
            moves = [(near + 1, near), (count - 2 - near, count - 1 - near)]
        arrived = lax.ppermute(total, "tensor", moves)
        if step < middle:
            total = lax.optimization_barrier(total + arrived)
        else:
            total = jnp.where((me == near) | (me == count - 1 - near), arrived, total)
            if step < count - 2:
                total = lax.optimization_barrier(total)
    return total


def per_device(
    shards,
    tensors,
    tokens,
    ln1_gain,
    ln1_bias,
    qkv_weight,
    qkv_bias,
    out_weight,
    out_bias,
    ln2_gain,
    ln2_bias,
    fc1_weight,
    fc1_bias,
    fc2_weight,
    fc2_bias,
    cotangent,
):
    own_rows, head_count, kinds, head_dim = qkv_weight.shape
    row_count, width = tokens.shape
    table = rotary_tables(SEQ, ROT)

    vectors = jnp.stack([ln1_gain, ln1_bias, ln2_gain, ln2_bias, out_bias, fc2_bias] + [ln1_gain] * 10)
    parts = [
        vectors,
        qkv_weight.reshape(own_rows, -1),
        fc1_weight,
        out_weight.reshape(own_rows, -1),
        fc2_weight,
    ]
    qkv_shift = qkv_bias.astype(jnp.float32).reshape(1, -1)
    fc1_shift = fc1_bias.astype(jnp.float32).reshape(1, -1)
    forward = None
    if ring_serves(shards):
        gathered, forward = gather_forward(
            parts, tokens, qkv_shift, fc1_shift, table, shards, head_count, head_dim
        )
    else:
        gathered = [lax.all_gather(part, "shard") for part in parts]
    vectors = gathered[0].astype(jnp.float32).transpose(1, 0, 2).reshape(16, width)
    qkv_full, fc1_full, out_full, fc2_full = (
        part.reshape(width, part.shape[-1]) for part in gathered[1:]
    )
    if forward is None:
        normed_one, normed_two, qkv, attn_out = attention_forward(
            tokens, vectors, qkv_full, qkv_shift, table, head_count, head_dim
        )
        pre_act = dot_nn(normed_two, fc1_full) + fc1_shift
        hidden = gelu_exact(pre_act).astype(jnp.bfloat16)
    else:
        normed_one, normed_two, qkv, attn_out, hidden, pre_act = forward

    block_out = lax.optimization_barrier(jnp.zeros((row_count, width), jnp.bfloat16))
    start = 0
    shifts = vectors[4] + vectors[5]
    for parts in FWD_PARTS:
        rows = row_count // parts
        partial_value = branch_part(attn_out, hidden, out_full, fc2_full, start, rows)
        branch_total = line_sum(partial_value, tensors).astype(jnp.float32)
        out_rows = tokens[start : start + rows].astype(jnp.float32) + branch_total + shifts
        block_out = lax.dynamic_update_slice(block_out, out_rows.astype(jnp.bfloat16), (start, 0))
        start += rows

    def weight_grad(left, right):
        return dot_tn(left, right).astype(jnp.bfloat16)

    def scattered(left, right):
        grad = weight_grad(left, right)
        grad = lax.psum_scatter(grad, "shard", scatter_dimension=0, tiled=True)
        return grad.astype(jnp.float32)

    grad_fc2 = scattered(cotangent, hidden)
    grad_out = scattered(cotangent, attn_out)
    d_pre = dot_nn(cotangent, fc2_full) * gelu_slope(pre_act)
    fc1_shift_grad = jnp.sum(d_pre, axis=0)
    d_pre = d_pre.astype(jnp.bfloat16)
    grad_fc1 = scattered(normed_two, d_pre)
    d_qkv, qkv_shift_grad, shift_grad = attention_backward(
        cotangent, out_full, qkv, table, head_count, head_dim
    )
    grad_qkv = scattered(normed_one, d_qkv)

    grad_tokens = lax.optimization_barrier(jnp.zeros((row_count, width), jnp.float32))
    norm_terms = 0.0
    start = 0
    for index, parts in enumerate(BWD_PARTS):
        rows = row_count // parts
        d_input, terms = input_grad(d_pre, d_qkv, tokens, vectors, fc1_full, qkv_full, start, rows)
        norm_terms = norm_terms + terms
        at = 0
        for cut in LAST_PARTS if index + 1 == len(BWD_PARTS) else (1,):
            sent = rows // cut
            piece = lax.optimization_barrier(d_input[at : at + sent]) if cut > 1 else d_input
            summed = line_sum(piece, tensors).astype(jnp.float32)
            grad_rows = cotangent[start + at : start + at + sent].astype(jnp.float32) + summed
            grad_tokens = lax.dynamic_update_slice(grad_tokens, grad_rows, (start + at, 0))
            at += sent
        start += rows

    shared = lax.psum(
        jnp.concatenate(
            [norm_terms[:4].reshape(-1), shift_grad[0], qkv_shift_grad[0], fc1_shift_grad]
        ),
        "shard",
    )
    columns = shared[: 5 * width].reshape(5, shards, own_rows)
    columns = lax.dynamic_index_in_dim(columns, lax.axis_index("shard"), axis=1, keepdims=False)
    column_terms = line_sum(jnp.tile(columns[:4], (2, 1)), tensors)
    shared = shared[5 * width :]
    qkv_terms = shared[: head_count * kinds * head_dim].reshape(qkv_bias.shape)
    fc1_terms = shared[head_count * kinds * head_dim :]
    return (
        block_out,
        grad_tokens,
        column_terms[0],
        column_terms[1],
        grad_qkv.reshape(qkv_weight.shape),
        qkv_terms,
        grad_out.reshape(out_weight.shape),
        columns[4],
        column_terms[2],
        column_terms[3],
        grad_fc1,
        fc1_terms,
        grad_fc2,
        columns[4],
    )


def solution(mesh):
    return jax.shard_map(
        functools.partial(per_device, mesh.shape["shard"], mesh.shape["tensor"]),
        mesh=mesh,
        in_specs=(
            P("shard", None),
            P("shard"),
            P("shard"),
            P("shard", "tensor", None, None),
            P("tensor", None, None),
            P("shard", "tensor", None),
            P("shard"),
            P("shard"),
            P("shard"),
            P("shard", "tensor"),
            P("tensor"),
            P("shard", "tensor"),
            P("shard"),
            P("shard", None),
        ),
        out_specs=(
            P("shard", None),
            P("shard", None),
            P("shard"),
            P("shard"),
            P("shard", "tensor", None, None),
            P("tensor", None, None),
            P("shard", "tensor", None),
            P("shard"),
            P("shard"),
            P("shard"),
            P("shard", "tensor"),
            P("tensor"),
            P("shard", "tensor"),
            P("shard"),
        ),
        check_vma=False,
    )
```

```python
import functools
import math

import jax
import jax.numpy as jnp
import numpy as np
from jax import lax
from jax.experimental import pallas as pl
from jax.experimental.pallas import tpu as pltpu
from jax.sharding import PartitionSpec as P


ROT = 64
SEQ = 256
CORES = 2
LANES = 128
CHUNKS = 4
FWD_CALLS = (1, 3)
BWD_CALLS = (2, 2)
VMEM_LIMIT = 60 << 20


NORM_EPS = 1e-05
ROOT_HALF = 0.7071067811865476
INV_ROOT_TWO_PI = 0.3989422804014327
MESH = pl.DeviceIdType.MESH


def normalize(residual):
    row_mean = jnp.mean(residual, axis=-1, keepdims=True)
    centered = residual - row_mean
    row_var = jnp.mean(centered * centered, axis=-1, keepdims=True)
    inv_std = lax.rsqrt(row_var + NORM_EPS)
    return (centered * inv_std, inv_std)


def gelu_exact(pre_act):
    return 0.5 * pre_act * (1.0 + lax.erf(pre_act * ROOT_HALF))


def gelu_slope(pre_act):
    return (
        0.5 * (1.0 + lax.erf(pre_act * ROOT_HALF))
        + pre_act * jnp.exp(-0.5 * pre_act * pre_act) * INV_ROOT_TWO_PI
    )


def rotary_tables(length, rot_dims):
    half_dims = rot_dims // 2
    frequency = 10000.0 ** (-2.0 * np.arange(half_dims) / rot_dims)
    angles = np.arange(length)[:, None] * frequency[None, :]
    cos_tab, sin_tab = np.cos(angles), np.sin(angles)
    tables = np.zeros((3, length, LANES), np.float32)
    tables[0] = 1.0
    tables[0, :, :half_dims] = cos_tab
    tables[0, :, half_dims:rot_dims] = cos_tab
    tables[1, :, :half_dims] = -sin_tab
    tables[2, :, half_dims:rot_dims] = sin_tab
    return jnp.asarray(tables)


def rotate(field, table_ref, sign):
    first = field[:, :LANES]
    half_dims = ROT // 2
    turned = (
        first * table_ref[0]
        + sign * pltpu.roll(first, LANES - half_dims, 1) * table_ref[1]
        + sign * pltpu.roll(first, half_dims, 1) * table_ref[2]
    )
    return jnp.concatenate([turned, field[:, LANES:]], axis=1)


def dot_nn(left, right):
    return jnp.dot(left, right, preferred_element_type=jnp.float32)


def dot_nt(left, right):
    return lax.dot_general(left, right, (((1,), (1,)), ((), ())), preferred_element_type=jnp.float32)


def dot_tn(left, right):
    return lax.dot_general(left, right, (((0,), (0,)), ((), ())), preferred_element_type=jnp.float32)


def probabilities(queries, key_rows, score_scale):
    scores = dot_nt(queries, key_rows) * score_scale
    length = scores.shape[0]
    row_at = lax.broadcasted_iota(jnp.int32, (length, length), 0)
    key_at = lax.broadcasted_iota(jnp.int32, (length, length), 1)
    scores = jnp.where(row_at >= key_at, scores, -1e30)
    row_top = jnp.max(scores, axis=-1, keepdims=True)
    weights = jnp.exp(scores - row_top)
    return weights * (1.0 / jnp.sum(weights, axis=-1, keepdims=True))


def call(kernel, grid, in_specs, out_specs, out_shape, flops, moved, **more):
    return pl.pallas_call(
        kernel,
        grid=grid,
        in_specs=in_specs,
        out_specs=out_specs,
        out_shape=out_shape,
        compiler_params=pltpu.CompilerParams(vmem_limit_bytes=VMEM_LIMIT),
        cost_estimate=pl.CostEstimate(flops=flops, bytes_accessed=moved, transcendentals=0),
        **more,
    )


def whole(shape):
    return pl.BlockSpec(
        shape, lambda step: (0,) * len(shape), pipeline_mode=pl.Buffered(1)
    )


def by_rows(rows, columns, first=0):
    return pl.BlockSpec((rows, columns), lambda step: (step + first, 0))


def chunk_specs(chunks, chunk_rows, columns):
    blocks = chunk_rows // SEQ
    return [
        pl.BlockSpec(
            (SEQ, columns),
            lambda step, chunk=chunk: (jnp.clip(step - chunk * blocks, 0, blocks - 1), 0),
        )
        for chunk in range(chunks)
    ]


def store_chunk(refs, chunk_rows, value):
    at = pl.program_id(0) // (chunk_rows // SEQ)
    for chunk, ref in enumerate(refs):

        @pl.when(at == chunk)
        def _(ref=ref):
            ref[...] = value


def attention_block(
    x_ref,
    vec_ref,
    weight_ref,
    shift_ref,
    table_ref,
    one_ref,
    two_ref,
    qkv_ref,
    attn_ref,
    head_count,
    head_dim,
):
    score_scale = 1.0 / math.sqrt(head_dim)
    normalized, _ = normalize(x_ref[...].astype(jnp.float32))
    one = (normalized * vec_ref[0:1] + vec_ref[1:2]).astype(jnp.bfloat16)
    one_ref[...] = one
    two_ref[...] = (normalized * vec_ref[2:3] + vec_ref[3:4]).astype(jnp.bfloat16)
    for head in range(head_count):
        fields = []
        for kind in range(3):
            at = slice((head * 3 + kind) * head_dim, (head * 3 + kind + 1) * head_dim)
            field = dot_nn(one, weight_ref[:, at]) + shift_ref[:, at]
            if kind < 2:
                field = rotate(field, table_ref, 1.0)
            field = field.astype(jnp.bfloat16)
            qkv_ref[:, at] = field
            fields.append(field)
        probs = probabilities(fields[0], fields[1], score_scale).astype(jnp.bfloat16)
        attn_ref[:, head * head_dim : (head + 1) * head_dim] = dot_nn(probs, fields[2]).astype(
            jnp.bfloat16
        )


def attention_forward(tokens, vectors, qkv_full, qkv_shift, table, head_count, head_dim):
    row_count, width = tokens.shape
    qkv_width = qkv_full.shape[1]

    def kernel(x_ref, vec_ref, weight_ref, shift_ref, table_ref, *out_refs):
        attention_block(
            x_ref, vec_ref, weight_ref, shift_ref, table_ref, *out_refs, head_count, head_dim
        )

    attn_width = head_count * head_dim
    return call(
        kernel,
        (row_count // SEQ,),
        [
            by_rows(SEQ, width),
            whole(vectors.shape),
            whole(qkv_full.shape),
            whole(qkv_shift.shape),
            whole(table.shape),
        ],
        [
            by_rows(SEQ, width),
            by_rows(SEQ, width),
            by_rows(SEQ, qkv_width),
            by_rows(SEQ, attn_width),
        ],
        [
            jax.ShapeDtypeStruct((row_count, width), jnp.bfloat16),
            jax.ShapeDtypeStruct((row_count, width), jnp.bfloat16),
            jax.ShapeDtypeStruct((row_count, qkv_width), jnp.bfloat16),
            jax.ShapeDtypeStruct((row_count, attn_width), jnp.bfloat16),
        ],
        2 * row_count * width * qkv_width,
        2 * (3 * row_count * width + width * qkv_width + row_count * (qkv_width + attn_width)),
        name="attention_forward",
    )(tokens, vectors, qkv_full, qkv_shift, table)


def attention_backward(cotangent, out_full, qkv, table, head_count, head_dim):
    row_count, width = cotangent.shape
    qkv_width = qkv.shape[1]
    attn_width = head_count * head_dim
    score_scale = 1.0 / math.sqrt(head_dim)

    def kernel(grad_ref, out_ref, qkv_ref, table_ref, d_qkv_ref, shift_ref, sum_ref):
        @pl.when(pl.program_id(0) == 0)
        def _():
            shift_ref[...] = jnp.zeros_like(shift_ref)
            sum_ref[...] = jnp.zeros_like(sum_ref)

        grad = grad_ref[...]
        sum_ref[0:1] += jnp.sum(grad.astype(jnp.float32), axis=0, keepdims=True)
        for head in range(head_count):
            d_attn = dot_nn(grad, out_ref[:, head * head_dim : (head + 1) * head_dim])
            d_attn = d_attn.astype(jnp.bfloat16)
            at = [
                slice((head * 3 + kind) * head_dim, (head * 3 + kind + 1) * head_dim)
                for kind in range(3)
            ]
            queries, key_rows, values = (qkv_ref[:, part] for part in at)
            probs = probabilities(queries, key_rows, score_scale)
            d_values = dot_tn(probs.astype(jnp.bfloat16), d_attn)
            d_probs = dot_nt(d_attn, values)
            row_delta = jnp.sum(probs * d_probs, axis=-1, keepdims=True)
            d_scores = (probs * (d_probs - row_delta) * score_scale).astype(jnp.bfloat16)
            d_queries = rotate(dot_nn(d_scores, key_rows), table_ref, -1.0)
            d_keys = rotate(dot_tn(d_scores, queries), table_ref, -1.0)
            for part, value in zip(at, (d_queries, d_keys, d_values)):
                d_qkv_ref[:, part] = value.astype(jnp.bfloat16)
                shift_ref[0:1, part] += jnp.sum(value, axis=0, keepdims=True)

    return call(
        kernel,
        (row_count // SEQ,),
        [by_rows(SEQ, width), whole(out_full.shape), by_rows(SEQ, qkv_width), whole(table.shape)],
        [
            by_rows(SEQ, qkv_width),
            pl.BlockSpec((8, qkv_width), lambda step: (0, 0)),
            pl.BlockSpec((8, width), lambda step: (0, 0)),
        ],
        [
            jax.ShapeDtypeStruct((row_count, qkv_width), jnp.bfloat16),
            jax.ShapeDtypeStruct((8, qkv_width), jnp.float32),
            jax.ShapeDtypeStruct((8, width), jnp.float32),
        ],
        2 * row_count * width * attn_width + 10 * row_count * SEQ * attn_width,
        2 * (row_count * width + width * attn_width + 2 * row_count * qkv_width),
        name="attention_backward",
    )(cotangent, out_full, qkv, table)


def branch_parts(attn_out, hidden, out_full, fc2_full, first, chunk_rows, chunks):
    width = out_full.shape[0]
    rows = chunk_rows * chunks

    def kernel(attn_ref, hidden_ref, out_ref, fc2_ref, *part_refs):
        total = dot_nt(attn_ref[...], out_ref[...]) + dot_nt(hidden_ref[...], fc2_ref[...])
        store_chunk(part_refs, chunk_rows, total.astype(jnp.bfloat16))

    inner = attn_out.shape[1] + hidden.shape[1]
    return call(
        kernel,
        (rows // SEQ,),
        [
            by_rows(SEQ, attn_out.shape[1], first // SEQ),
            by_rows(SEQ, hidden.shape[1], first // SEQ),
            whole(out_full.shape),
            whole(fc2_full.shape),
        ],
        chunk_specs(chunks, chunk_rows, width),
        [jax.ShapeDtypeStruct((chunk_rows, width), jnp.bfloat16)] * chunks,
        2 * rows * width * inner,
        2 * (rows * (width + inner) + width * inner),
        name="branch_parts",
    )(attn_out, hidden, out_full, fc2_full)


def input_grads(d_pre, d_qkv, tokens, vectors, fc1_full, qkv_full, first, chunk_rows, chunks):
    width = tokens.shape[1]
    rows = chunk_rows * chunks
    tile = min(width, 512)

    def kernel(pre_ref, qkv_ref, x_ref, vec_ref, fc1_ref, weight_ref, *refs):
        grad_refs, terms_ref, joined_ref = refs[:chunks], refs[chunks], refs[chunks + 1]

        @pl.when(pl.program_id(0) == 0)
        def _():
            terms_ref[...] = jnp.zeros_like(terms_ref)

        normalized, inv_std = normalize(x_ref[...].astype(jnp.float32))
        total = along = 0.0
        for at in range(0, width, tile):
            cut = slice(at, at + tile)
            norm_cut = normalized[:, cut]
            d_one = dot_nt(qkv_ref[...], weight_ref[cut])
            d_two = dot_nt(pre_ref[...], fc1_ref[cut])
            terms_ref[0:1, cut] += jnp.sum(d_one * norm_cut, axis=0, keepdims=True)
            terms_ref[1:2, cut] += jnp.sum(d_one, axis=0, keepdims=True)
            terms_ref[2:3, cut] += jnp.sum(d_two * norm_cut, axis=0, keepdims=True)
            terms_ref[3:4, cut] += jnp.sum(d_two, axis=0, keepdims=True)
            joined = d_one * vec_ref[0:1, cut] + d_two * vec_ref[2:3, cut]
            joined_ref[:, cut] = joined
            total += jnp.sum(joined, axis=-1, keepdims=True)
            along += jnp.sum(joined * norm_cut, axis=-1, keepdims=True)
        grad = inv_std * (joined_ref[...] - total / width - normalized * (along / width))
        store_chunk(grad_refs, chunk_rows, grad.astype(jnp.bfloat16))

    inner = d_pre.shape[1] + d_qkv.shape[1]
    results = call(
        kernel,
        (rows // SEQ,),
        [
            by_rows(SEQ, d_pre.shape[1], first // SEQ),
            by_rows(SEQ, d_qkv.shape[1], first // SEQ),
            by_rows(SEQ, width, first // SEQ),
            whole(vectors.shape),
            whole(fc1_full.shape),
            whole(qkv_full.shape),
        ],
        chunk_specs(chunks, chunk_rows, width) + [pl.BlockSpec((8, width), lambda step: (0, 0))],
        [jax.ShapeDtypeStruct((chunk_rows, width), jnp.bfloat16)] * chunks
        + [jax.ShapeDtypeStruct((8, width), jnp.float32)],
        2 * rows * width * inner,
        2 * (rows * (2 * width + inner) + width * inner),
        scratch_shapes=[pltpu.VMEM((SEQ, width), jnp.float32)],
        name="input_grads",
    )(d_pre, d_qkv, tokens, vectors, fc1_full, qkv_full)
    return results[:chunks], results[chunks]


def chip_at(place, chips):
    if chips & (chips - 1):
        return place
    chip, bit = 0, 1
    while bit < chips:
        chip = chip + bit * lax.rem(place // bit + place // (2 * bit), 2)
        bit *= 2
    return chip


def place_of(chip, chips):
    if chips & (chips - 1):
        return chip
    place, bit = 0, 1
    while bit < chips:
        ones, higher = 0, bit
        while higher < chips:
            ones = ones + chip // higher
            higher *= 2
        place = place + bit * lax.rem(ones, 2)
        bit *= 2
    return place


def ring_serves(shards):
    chips = shards // CORES
    return shards % CORES == 0 and chips % 2 == 0 and chips >= 4


def gather_forward(parts, tokens, qkv_shift, fc1_shift, table, shards, head_count, head_dim):
    chips = shards // CORES
    count = len(parts)
    hops = chips // 2 - 1
    kinds = 2 * hops + 2
    total_kinds = kinds + 1 + kinds
    row_count, width = tokens.shape
    own_rows, qkv_width = parts[1].shape
    units = parts[2].shape[1]
    attn_width = head_count * head_dim

    def kernel(*refs):
        own = refs[:count]
        x_ref, qkv_shift_ref, fc1_shift_ref, table_ref = refs[count : count + 4]
        full = refs[count + 4 : 2 * count + 4]
        one_ref, two_ref, qkv_ref, attn_ref, hidden_ref, pre_ref = refs[2 * count + 4 : 2 * count + 10]
        vec_buf, vec_rows, qkv_buf, fc1_buf, send_sems, recv_sems, keep_sems, load_sems = refs[
            2 * count + 10 :
        ]
        me = lax.axis_index("shard")
        core = lax.rem(me, CORES)
        place = place_of(me // CORES, chips)

        def shard_at(shift, flip=0):
            there = chip_at(lax.rem(place + shift + chips, chips), chips)
            return there * CORES + (1 - core if flip else core)

        right, left, peer = shard_at(1), shard_at(-1), shard_at(0, 1)
        barrier = pltpu.get_barrier_semaphore()
        for target in (right, left, peer):
            pl.semaphore_signal(barrier, inc=1, device_id={"shard": target}, device_id_type=MESH)
        pl.semaphore_wait(barrier, 3)
        copies = {}

        def send(index, kind, src, dst, target):
            copy = pltpu.make_async_remote_copy(
                src_ref=src,
                dst_ref=dst,
                send_sem=send_sems.at[index, kind],
                recv_sem=recv_sems.at[index, kind],
                device_id={"shard": target},
                device_id_type=MESH,
            )
            copy.start()
            copies[index, kind] = copy

        def half(which, index):
            rows = own[index].shape[0] // 2
            return pl.ds(which * rows, rows)

        def across(index, kind, piece):
            send(index, kinds + 1 + kind, piece, piece, peer)

        def keep(index):
            return pltpu.make_async_copy(own[index], full[index].at[me], keep_sems.at[index])

        def begin(*indices):
            for index in indices:
                mine = full[index].at[me]
                send(index, 0, own[index], mine, right)
                send(index, hops, own[index], mine, left)
                send(index, kinds, own[index], mine, peer)
                keep(index).start()

        def forward(*indices):
            for hop in range(hops):
                for index in indices:
                    for kind, sign, target in ((hop, -1, right), (hops + hop, 1, left)):
                        copies[index, kind].wait_recv()
                        shard = shard_at(sign * (hop + 1))
                        piece = full[index].at[shard]
                        if hop + 1 < hops:
                            send(index, kind + 1, piece, piece, target)
                        else:
                            which = 0 if sign < 0 else 1
                            part = full[index].at[shard, half(which, index)]
                            send(index, 2 * hops + which, part, part, target)
                        across(index, kind, piece)

        def finish(*indices):
            for index in indices:
                for which in range(2):
                    last = 2 * hops + which
                    copies[index, last].wait_recv()
                    across(index, last, full[index].at[shard_at(chips // 2), half(which, index)])
            for index in indices:
                for kind in range(kinds, total_kinds):
                    copies[index, kind].wait_recv()
                for kind in range(total_kinds):
                    copies[index, kind].wait_send()
                keep(index).wait()

        def load(index, buffer, slot):
            loads = [
                pltpu.make_async_copy(
                    full[index].at[shard],
                    buffer.at[pl.ds(shard * own[index].shape[0], own[index].shape[0])],
                    load_sems.at[slot + shard],
                )
                for shard in range(shards)
            ]
            for one in loads:
                one.start()
            for one in loads:
                one.wait()

        def pipeline(body, half_at, taken, made, *arrays):
            steps = row_count // SEQ // 2

            def rows_of(columns):
                return pl.BlockSpec((SEQ, columns), lambda step: (step + half_at * steps, 0))

            pltpu.emit_pipeline(
                body,
                grid=(steps,),
                in_specs=[rows_of(columns) for columns in taken],
                out_specs=[rows_of(columns) for columns in made],
            )(*arrays)

        begin(0, 1)
        forward(0, 1)
        begin(2, 3)
        finish(0, 1)
        load(0, vec_buf, 0)
        load(1, qkv_buf, shards)
        for shard in range(shards):
            vec_rows[:, shard * own_rows : (shard + 1) * own_rows] = vec_buf[
                shard * 16 : (shard + 1) * 16
            ].astype(jnp.float32)

        def attend(*blocks):
            attention_block(
                blocks[0],
                vec_rows,
                qkv_buf,
                qkv_shift_ref,
                table_ref,
                *blocks[1:],
                head_count,
                head_dim,
            )

        def attend_half(half_at):
            pipeline(
                attend,
                half_at,
                [width],
                [width, width, qkv_width, attn_width],
                x_ref,
                one_ref,
                two_ref,
                qkv_ref,
                attn_ref,
            )

        attend_half(0)
        forward(2)
        begin(4)
        attend_half(1)
        finish(2)
        load(2, fc1_buf, 2 * shards)

        def feed(two_block, hidden_block, pre_block):
            tile = min(units, 512)
            for at in range(0, units, tile):
                cut = slice(at, at + tile)
                pre = dot_nn(two_block[...], fc1_buf[:, cut]) + fc1_shift_ref[:, cut]
                pre_block[:, cut] = pre
                hidden_block[:, cut] = gelu_exact(pre).astype(jnp.bfloat16)

        pipeline(feed, 0, [width], [units, units], two_ref, hidden_ref, pre_ref)
        forward(3, 4)
        pipeline(feed, 1, [width], [units, units], two_ref, hidden_ref, pre_ref)
        finish(3, 4)

    sent = sum(part.size * part.dtype.itemsize for part in parts)
    any_space = pl.BlockSpec(memory_space=pl.ANY)
    in_vmem = pl.BlockSpec(memory_space=pltpu.VMEM)
    shapes = [((shards,) + part.shape, part.dtype) for part in parts] + [
        ((row_count, width), jnp.bfloat16),
        ((row_count, width), jnp.bfloat16),
        ((row_count, qkv_width), jnp.bfloat16),
        ((row_count, attn_width), jnp.bfloat16),
        ((row_count, units), jnp.bfloat16),
        ((row_count, units), jnp.float32),
    ]
    results = pl.pallas_call(
        kernel,
        in_specs=[in_vmem] * count + [any_space] + [in_vmem] * 3,
        out_specs=[any_space] * len(shapes),
        out_shape=[jax.ShapeDtypeStruct(*shape) for shape in shapes],
        scratch_shapes=[
            pltpu.VMEM((shards * 16, own_rows), jnp.bfloat16),
            pltpu.VMEM((16, width), jnp.float32),
            pltpu.VMEM((width, qkv_width), jnp.bfloat16),
            pltpu.VMEM((width, units), jnp.bfloat16),
            pltpu.SemaphoreType.DMA((count, total_kinds)),
            pltpu.SemaphoreType.DMA((count, total_kinds)),
            pltpu.SemaphoreType.DMA((count,)),
            pltpu.SemaphoreType.DMA((3 * shards,)),
        ],
        compiler_params=pltpu.CompilerParams(
            collective_id=0, has_side_effects=True, vmem_limit_bytes=VMEM_LIMIT
        ),
        cost_estimate=pl.CostEstimate(
            flops=2 * row_count * width * (qkv_width + units),
            bytes_accessed=2 * shards * sent + 18 * row_count * width,
            transcendentals=row_count * units,
        ),
        name="gather_forward",
    )(*parts, tokens, qkv_shift, fc1_shift, table)
    return results[:count], results[count:]


def line_sum(part, count):
    if count == 1:
        return part
    if count % 2:
        return lax.psum(part, "tensor")
    me = lax.axis_index("tensor")
    middle = count // 2
    total = part
    for step in range(count - 1):
        if step < middle:
            moves = [(step, step + 1), (count - 1 - step, count - 2 - step)]
        else:
            near = count - 2 - step
            moves = [(near + 1, near), (count - 2 - near, count - 1 - near)]
        arrived = lax.ppermute(total, "tensor", moves)
        if step < middle:
            total = lax.optimization_barrier(total + arrived)
        else:
            total = jnp.where((me == near) | (me == count - 1 - near), arrived, total)
            if step < count - 2:
                total = lax.optimization_barrier(total)
    return total


def per_device(
    shards,
    tensors,
    tokens,
    ln1_gain,
    ln1_bias,
    qkv_weight,
    qkv_bias,
    out_weight,
    out_bias,
    ln2_gain,
    ln2_bias,
    fc1_weight,
    fc1_bias,
    fc2_weight,
    fc2_bias,
    cotangent,
):
    own_rows, head_count, kinds, head_dim = qkv_weight.shape
    row_count, width = tokens.shape
    table = rotary_tables(SEQ, ROT)

    vectors = jnp.stack([ln1_gain, ln1_bias, ln2_gain, ln2_bias, out_bias, fc2_bias] + [ln1_gain] * 10)
    parts = [
        vectors,
        qkv_weight.reshape(own_rows, -1),
        fc1_weight,
        out_weight.reshape(own_rows, -1),
        fc2_weight,
    ]
    qkv_shift = qkv_bias.astype(jnp.float32).reshape(1, -1)
    fc1_shift = fc1_bias.astype(jnp.float32).reshape(1, -1)
    forward = None
    if ring_serves(shards):
        gathered, forward = gather_forward(
            parts, tokens, qkv_shift, fc1_shift, table, shards, head_count, head_dim
        )
    else:
        gathered = [lax.all_gather(part, "shard") for part in parts]
    vectors = gathered[0].astype(jnp.float32).transpose(1, 0, 2).reshape(16, width)
    qkv_full, fc1_full, out_full, fc2_full = (
        part.reshape(width, part.shape[-1]) for part in gathered[1:]
    )
    if forward is None:
        normed_one, normed_two, qkv, attn_out = attention_forward(
            tokens, vectors, qkv_full, qkv_shift, table, head_count, head_dim
        )
        pre_act = dot_nn(normed_two, fc1_full) + fc1_shift
        hidden = gelu_exact(pre_act).astype(jnp.bfloat16)
    else:
        normed_one, normed_two, qkv, attn_out, hidden, pre_act = forward

    block_out = lax.optimization_barrier(jnp.zeros((row_count, width), jnp.bfloat16))
    chunk_rows = row_count // CHUNKS
    shifts = vectors[4] + vectors[5]
    chunk = 0
    for made in FWD_CALLS:
        pieces = branch_parts(
            attn_out, hidden, out_full, fc2_full, chunk * chunk_rows, chunk_rows, made
        )
        for piece in pieces:
            start = chunk * chunk_rows
            branch_total = line_sum(piece, tensors).astype(jnp.float32)
            out_rows = tokens[start : start + chunk_rows].astype(jnp.float32)
            out_rows = (out_rows + branch_total + shifts).astype(jnp.bfloat16)
            block_out = lax.dynamic_update_slice(block_out, out_rows, (start, 0))
            chunk += 1

    def weight_grad(left, right):
        return dot_tn(left, right).astype(jnp.bfloat16)

    def scattered(left, right, like):
        grad = weight_grad(left, right)
        grad = lax.psum_scatter(grad, "shard", scatter_dimension=0, tiled=True)
        return grad.astype(jnp.float32).reshape(like.shape)

    grad_fc2 = scattered(cotangent, hidden, fc2_weight)
    grad_out = scattered(cotangent, attn_out, out_weight)
    d_pre = dot_nn(cotangent, fc2_full) * gelu_slope(pre_act)
    fc1_shift_grad = jnp.sum(d_pre, axis=0)
    d_pre = d_pre.astype(jnp.bfloat16)
    grad_fc1 = scattered(normed_two, d_pre, fc1_weight)
    d_qkv, qkv_shift_grad, shift_grad = attention_backward(
        cotangent, out_full, qkv, table, head_count, head_dim
    )
    grad_qkv = scattered(normed_one, d_qkv, qkv_weight)

    grad_tokens = lax.optimization_barrier(jnp.zeros((row_count, width), jnp.float32))
    norm_terms = 0.0
    start = 0
    for made in BWD_CALLS:
        pieces, terms = input_grads(
            d_pre, d_qkv, tokens, vectors, fc1_full, qkv_full, start, chunk_rows, made
        )
        norm_terms = norm_terms + terms
        for piece in pieces:
            summed = line_sum(piece, tensors).astype(jnp.float32)
            grad_rows = cotangent[start : start + chunk_rows].astype(jnp.float32) + summed
            grad_tokens = lax.dynamic_update_slice(grad_tokens, grad_rows, (start, 0))
            start += chunk_rows
            chunk += 1

    shared = lax.psum(
        jnp.concatenate(
            [norm_terms[:4].reshape(-1), shift_grad[0], qkv_shift_grad[0], fc1_shift_grad]
        ),
        "shard",
    )
    columns = shared[: 5 * width].reshape(5, shards, own_rows)
    columns = lax.dynamic_index_in_dim(columns, lax.axis_index("shard"), axis=1, keepdims=False)
    column_terms = line_sum(jnp.tile(columns[:4], (2, 1)), tensors)
    shared = shared[5 * width :]
    qkv_terms = shared[: head_count * kinds * head_dim].reshape(qkv_bias.shape)
    fc1_terms = shared[head_count * kinds * head_dim :]
    return (
        block_out,
        grad_tokens,
        column_terms[0],
        column_terms[1],
        grad_qkv,
        qkv_terms,
        grad_out,
        columns[4],
        column_terms[2],
        column_terms[3],
        grad_fc1,
        fc1_terms,
        grad_fc2,
        columns[4],
    )


def solution(mesh):
    return jax.shard_map(
        functools.partial(per_device, mesh.shape["shard"], mesh.shape["tensor"]),
        mesh=mesh,
        in_specs=(
            P("shard", None),
            P("shard"),
            P("shard"),
            P("shard", "tensor", None, None),
            P("tensor", None, None),
            P("shard", "tensor", None),
            P("shard"),
            P("shard"),
            P("shard"),
            P("shard", "tensor"),
            P("tensor"),
            P("shard", "tensor"),
            P("shard"),
            P("shard", None),
        ),
        out_specs=(
            P("shard", None),
            P("shard", None),
            P("shard"),
            P("shard"),
            P("shard", "tensor", None, None),
            P("tensor", None, None),
            P("shard", "tensor", None),
            P("shard"),
            P("shard"),
            P("shard"),
            P("shard", "tensor"),
            P("tensor"),
            P("shard", "tensor"),
            P("shard"),
        ),
        check_vma=False,
    )
```
